32 devices in a mesh: dp: 8 (over z, x), blk: 4 (over y, core).
Axes of the slice: x: 2, y: 2, z: 4, core: 2. Of those that a mesh axis runs over, the one named last changes fastest.
Arguments:
- queries: bfloat16 [8, 512, 2048], P('dp', 'blk'), may hold values from -6 to 6
- keys: bfloat16 [8, 512, 512], P('dp', 'blk'), may hold values from -6 to 6
- values: bfloat16 [8, 512, 512], P('dp', 'blk'), may hold values from -6 to 6
- out_grad: bfloat16 [8, 512, 2048], P('dp', 'blk'), may hold values from -6 to 6
- layer_input: bfloat16 [8, 512, 4096], P('dp', 'blk'), may hold values from -6 to 6
- lengths: int32 [8, 3], P('dp'), may hold values from 32 to 448, as said below
Outputs:
- query_grad: bfloat16 [8, 512, 2048], P('dp', 'blk')
- key_grad: bfloat16 [8, 512, 512], P('dp', 'blk')
- value_grad: bfloat16 [8, 512, 512], P('dp', 'blk')
- weight_grad: float32 [4096, 1024], P(('dp', 'blk'))
The draws below stay inside these ranges and needn't reach their ends.
Inputs may be any that keep to these rules, and one draw needn't show every extreme that they name: `lengths`: each row sums to 512; the chosen and rejected counts lie between 32 and 96.
All inputs are finite; a program needn't handle non-finite values.
Results may differ from the reference program's by a relative error of at most 0.023.
Values may be sent and summed in bfloat16 or wider, within the bound.
No kernel may reach another device: no remote copies, remote signals or barrier semaphores. Data moves between devices by JAX's collectives and lax.ppermute only.
A program may use at most 128 MiB of HBM per device.

```python
import math
import jax
import jax.numpy as jnp
from jax import lax

D = 4096
H = 16
KV = 4
HEAD = 128
TOK_DEV = 128
SEQ_LEN = 512
SEQS = 8
N_BLK = 4


def draw_queries(key, part):
    own_key = jax.random.fold_in(key, 1)
    normal_key = jax.random.fold_in(own_key, 0)
    values_drawn = jax.random.normal(normal_key, (SEQS, SEQ_LEN, H * HEAD), jnp.float32)
    return jnp.clip(values_drawn, -6.0, 6.0).astype(jnp.bfloat16)


def draw_keys(key, part):
    own_key = jax.random.fold_in(key, 2)
    normal_key = jax.random.fold_in(own_key, 0)
    values_drawn = jax.random.normal(normal_key, (SEQS, SEQ_LEN, KV * HEAD), jnp.float32)
    return jnp.clip(values_drawn, -6.0, 6.0).astype(jnp.bfloat16)


def draw_lengths(key, part):
    first_key, second_key = jax.random.split(jax.random.fold_in(key, 5))
    lowest = SEQ_LEN // 16
    highest = 3 * SEQ_LEN // 16 + 1
    chosen_len = jax.random.randint(first_key, (SEQS,), lowest, highest)
    rejected_len = jax.random.randint(second_key, (SEQS,), lowest, highest)
    prompt_len = SEQ_LEN - chosen_len - rejected_len
    return jnp.stack([prompt_len, chosen_len, rejected_len], axis=1).astype(jnp.int32)


def block_levels(key, dims, pieces, least, top_value):
    def one(axis_at, parts):
        draws = jax.random.uniform(jax.random.fold_in(jax.random.fold_in(key, 6), axis_at), (parts,), jnp.float32, least / len(pieces), top_value / len(pieces))
        return jnp.repeat(jnp.exp(draws), dims[axis_at] // parts).reshape((-1,) + (1,) * (len(dims) - axis_at - 1))

    loudness = one(*pieces[0])
    for cut in pieces[1:]:
        loudness = loudness * one(*cut)
    return loudness


def normal_values(rng, shape, deviation, bound, cuts=(), kind=jnp.bfloat16):
    level = block_levels(rng, shape, cuts, -0.22, 0.18) if cuts else 1.0
    entries = jax.random.normal(rng, shape, jnp.float32) * deviation * level
    return jnp.minimum(jnp.maximum(entries, -bound), bound).astype(kind)


def setup_inputs(seed: int = 0) -> dict:
    key_list = jax.random.split(jax.random.key(seed), 7)
    return {
        "queries": draw_queries(jax.random.fold_in(key_list[6], 71), 0),
        "keys": draw_keys(jax.random.fold_in(key_list[6], 71), 0),
        "values": normal_values(key_list[2], (SEQS, SEQ_LEN, KV * HEAD), 1.0, 6.0, ((0, 8), (1, 4))),
        "out_grad": normal_values(key_list[3], (SEQS, SEQ_LEN, H * HEAD), 1.0, 6.0, ((0, 8), (1, 4))),
        "layer_input": normal_values(key_list[4], (SEQS, SEQ_LEN, D), 1.0, 6.0, ((0, 8), (1, 4))),
        "lengths": draw_lengths(jax.random.fold_in(key_list[6], 71), 0),
    }


rope_base = 500000.0
masked_fill = -1e+30

def stored_positions(stored_rows, shard_rows, shard_count):
    half_rows = shard_rows // 2
    block_number = stored_rows // half_rows
    holder = block_number // 2
    upper_half = block_number % 2
    position_block = jnp.where(upper_half == 1, 2 * shard_count - 1 - holder, holder)
    return (position_block * half_rows + stored_rows % half_rows).astype(jnp.int32)

def allowed_pairs(query_pos, key_pos, prompt_len, chosen_len):
    causal = key_pos[None, :] <= query_pos[:, None]
    reject_start = prompt_len + chosen_len
    query_rejected = query_pos >= reject_start
    key_chosen = jnp.logical_and(key_pos >= prompt_len, key_pos < reject_start)
    return jnp.logical_and(causal, jnp.logical_not(jnp.logical_and(query_rejected[:, None], key_chosen[None, :])))

def rope_inverse(grad_sum, positions):
    half_dim = HEAD // 2
    frequency = jnp.exp(-(2.0 * jnp.arange(half_dim, dtype=jnp.float32) / HEAD) * math.log(rope_base))
    angles = positions.astype(jnp.float32)[:, None] * frequency[None, :]
    cosine = jnp.concatenate([jnp.cos(angles), jnp.cos(angles)], axis=-1)[:, None, :]
    sine = jnp.concatenate([jnp.sin(angles), jnp.sin(angles)], axis=-1)[:, None, :]
    grad_heads = grad_sum.reshape(grad_sum.shape[0], -1, HEAD)
    rotated = jnp.concatenate([-grad_heads[..., half_dim:], grad_heads[..., :half_dim]], axis=-1)
    return (grad_heads * cosine - rotated * sine).reshape(grad_sum.shape[0], -1).astype(jnp.bfloat16)

def one_sequence(operands):
    queries, keys, values, out_grad, lengths = operands
    seq_len = queries.shape[0]
    group_heads = H // KV
    scale = 1.0 / math.sqrt(HEAD)
    positions = stored_positions(jnp.arange(seq_len, dtype=jnp.int32), TOK_DEV, N_BLK)
    allowed = allowed_pairs(positions, positions, lengths[0], lengths[1])
    query_heads = queries.reshape(seq_len, KV, group_heads, HEAD).transpose(1, 2, 0, 3).astype(jnp.float32)
    grad_heads = out_grad.reshape(seq_len, KV, group_heads, HEAD).transpose(1, 2, 0, 3).astype(jnp.float32)
    key_heads = keys.reshape(seq_len, KV, HEAD).transpose(1, 0, 2).astype(jnp.float32)
    value_heads = values.reshape(seq_len, KV, HEAD).transpose(1, 0, 2).astype(jnp.float32)

    def one_group(group_operands):
        group_query, group_key, group_value, group_grad = group_operands
        scores = scale * jnp.einsum('hqe,ke->hqk', group_query, group_key)
        row_max = lax.optimization_barrier(jnp.max(jnp.where(allowed[None], scores, masked_fill), axis=-1))
        weights = jnp.where(allowed[None], jnp.exp(scores - row_max[..., None]), 0.0)
        row_sum = lax.optimization_barrier(jnp.sum(weights, axis=-1))
        attn_out = jnp.einsum('hqk,ke->hqe', weights, group_value, precision=lax.Precision.HIGHEST) / row_sum[..., None]
        log_total = row_max + jnp.log(row_sum)
        delta = lax.optimization_barrier(jnp.sum(group_grad * attn_out, axis=-1))
        probs = jnp.where(allowed[None], jnp.exp(scores - log_total[..., None]), 0.0)
        prob_half = probs.astype(jnp.bfloat16)
        prob_grad = jnp.einsum('hqe,ke->hqk', group_grad, group_value)
        score_grad = (scale * probs * (prob_grad - delta[..., None])).astype(jnp.bfloat16)
        query_grad = jnp.einsum('hqk,ke->hqe', score_grad.astype(jnp.float32), group_key)
        score_shards = score_grad.astype(jnp.float32).reshape(group_heads, N_BLK, TOK_DEV, seq_len)
        prob_shards = prob_half.astype(jnp.float32).reshape(group_heads, N_BLK, TOK_DEV, seq_len)
        query_shards = group_query.reshape(group_heads, N_BLK, TOK_DEV, HEAD)
        grad_shards = group_grad.reshape(group_heads, N_BLK, TOK_DEV, HEAD)
        key_parts = lax.optimization_barrier(jnp.einsum('hdqk,hdqe->dke', score_shards, query_shards).astype(jnp.bfloat16))
        value_parts = lax.optimization_barrier(jnp.einsum('hdqk,hdqe->dke', prob_shards, grad_shards).astype(jnp.bfloat16))
        key_sum = lax.optimization_barrier(jnp.sum(key_parts.astype(jnp.float32), axis=0))
        value_sum = lax.optimization_barrier(jnp.sum(value_parts.astype(jnp.float32), axis=0))
        return (query_grad, key_sum, value_sum)
    query_grad, key_sum, value_sum = lax.map(one_group, (query_heads, key_heads, value_heads, grad_heads))
    query_grad = query_grad.transpose(2, 0, 1, 3).reshape(seq_len, H * HEAD).astype(jnp.bfloat16)
    key_sum = key_sum.transpose(1, 0, 2).reshape(seq_len, KV * HEAD)
    value_sum = value_sum.transpose(1, 0, 2).reshape(seq_len, KV * HEAD)
    key_pre = rope_inverse(key_sum, positions)
    value_grad = value_sum.astype(jnp.bfloat16)
    grad_cols = jnp.concatenate([key_pre, value_grad], axis=1)
    return (query_grad, key_sum.astype(jnp.bfloat16), value_grad, grad_cols)

def reference(queries, keys, values, out_grad, layer_input, lengths):
    query_grad, key_grad, value_grad, grad_cols = lax.map(one_sequence, (queries, keys, values, out_grad, lengths))
    features = layer_input.shape[2]
    weight_grad = jnp.dot(layer_input.reshape(-1, features).T, grad_cols.reshape(-1, grad_cols.shape[2]), preferred_element_type=jnp.float32)
    return (query_grad, key_grad, value_grad, weight_grad)
```

```python
import functools
import math

import jax
import jax.numpy as jnp
from jax import lax
from jax.experimental import pallas as pl
from jax.experimental.pallas import tpu as pltpu
from jax.sharding import PartitionSpec as P

HEAD = 128
rope_base = 500000.0
masked_fill = -1e30
LOG2E = math.log2(math.e)
CHUNKS = 1
VMEM_LIMIT = 56 * 1024 * 1024


def stored_positions(stored_rows, shard_rows, shard_count):
    half_rows = shard_rows // 2
    block_number = stored_rows // half_rows
    holder = block_number // 2
    upper_half = block_number % 2
    position_block = jnp.where(upper_half == 1, 2 * shard_count - 1 - holder, holder)
    return (position_block * half_rows + stored_rows % half_rows).astype(jnp.int32)


def spread(index, bits):
    width = len(bits)
    return sum(((index >> (width - 1 - i)) & 1) << bits[i] for i in range(width))


class Exchange:
    def __init__(self, dp_count, blk_count):
        self.dp_count, self.blk_count = dp_count, blk_count
        self.blk_bits = blk_count.bit_length() - 1

    def __call__(self, array, mask):
        blk_mask, dp_mask = mask % self.blk_count, mask // self.blk_count
        if dp_mask == 0:
            return lax.ppermute(array, "blk", [(b, b ^ blk_mask) for b in range(self.blk_count)])
        if blk_mask == 0:
            return lax.ppermute(array, "dp", [(d, d ^ dp_mask) for d in range(self.dp_count)])
        total = self.dp_count * self.blk_count
        return lax.ppermute(array, ("dp", "blk"), [(i, i ^ mask) for i in range(total)])


def cost(flops, nbytes, trans=0):
    return pl.CostEstimate(flops=int(flops), bytes_accessed=int(nbytes), transcendentals=int(trans))


def turn_kernel(count, table_ref, *refs):
    del table_ref
    for m in range(count):
        refs[count + m][...] = refs[m][...].T


def turned_input(rows, table):
    row_count, features = rows.shape
    dests, blocks, share = table.shape[0], table.shape[1], None
    share = features // (dests * blocks)
    if share % 128:
        turned = rows.T.reshape(dests * blocks, share, row_count)
        return [turned[table[m]].reshape(blocks * share, row_count) for m in range(dests)]

    def source(m):
        return pl.BlockSpec((row_count, share), lambda r, t: (0, t[m, r]))

    out_spec = pl.BlockSpec((share, row_count), lambda r, t: (r, 0))
    return pl.pallas_call(
        functools.partial(turn_kernel, dests),
        grid_spec=pltpu.PrefetchScalarGridSpec(
            num_scalar_prefetch=1,
            grid=(blocks,),
            in_specs=[source(m) for m in range(dests)],
            out_specs=[out_spec] * dests,
        ),
        out_shape=[jax.ShapeDtypeStruct((blocks * share, row_count), rows.dtype)] * dests,
        cost_estimate=cost(1e9, 2 * rows.size * 2),
        name="turn",
    )(table, *[rows] * dests)


def attention_kernel(count, blk_count, group_heads, scale, meta_ref, *refs):
    key_refs, value_refs = refs[:count], refs[count : 2 * count]
    query_ref, grad_ref = refs[2 * count : 2 * count + 2]
    dquery_ref, keep_k, keep_v, send_k, send_v, bias_ref = refs[2 * count + 2 :]
    shard_rows = query_ref.shape[0]
    half = shard_rows // 2

    @pl.when(pl.program_id(0) == 0)
    def _():
        def positions(shard, local):
            low = shard * half + local
            high = (2 * blk_count - 1 - shard) * half + local - half
            return jnp.where(local < half, low, high)

        reject = meta_ref[count] + meta_ref[count + 1]
        shape = (shard_rows, shard_rows)
        query_pos = positions(meta_ref[0], lax.broadcasted_iota(jnp.int32, shape, 1))
        local = lax.broadcasted_iota(jnp.int32, shape, 0)
        for m in range(count):
            key_pos = positions(meta_ref[m], local)
            chosen = (key_pos >= meta_ref[count]) & (key_pos < reject)
            blocked = (key_pos > query_pos) | ((query_pos >= reject) & chosen)
            bias_ref[m * shard_rows : (m + 1) * shard_rows, :] = jnp.where(
                blocked, masked_fill, 0.0
            )

    def stacked(ref):
        return jnp.concatenate([ref[:, h * HEAD : (h + 1) * HEAD] for h in range(group_heads)], 0)

    query, grad = stacked(query_ref), stacked(grad_ref)
    key = jnp.concatenate([r[...] for r in key_refs], 0)
    value = jnp.concatenate([r[...] for r in value_refs], 0)
    contract_last = (((1,), (1,)), ((), ()))
    scores = lax.dot_general(key, query, contract_last, preferred_element_type=jnp.float32)
    prob_grad = lax.dot_general(value, grad, contract_last, preferred_element_type=jnp.float32)
    bias = bias_ref[...]
    scores = scores * (scale * LOG2E) + jnp.concatenate([bias] * group_heads, 1)
    row_max = jnp.max(scores, axis=0, keepdims=True)
    weights = jnp.exp2(scores - row_max)
    inverse = 1.0 / jnp.sum(weights, axis=0, keepdims=True)
    probs = weights * inverse
    delta = jnp.sum(probs * prob_grad, axis=0, keepdims=True)
    score_grad = ((probs * scale) * (prob_grad - delta)).astype(jnp.bfloat16)
    prob_half = probs.astype(jnp.bfloat16)
    plain = (((1,), (0,)), ((), ()))
    dvalue = lax.dot_general(prob_half, grad, plain, preferred_element_type=jnp.float32)
    dkey = lax.dot_general(score_grad, query, plain, preferred_element_type=jnp.float32)
    turned = lax.dot_general(
        key, score_grad, (((0,), (0,)), ((), ())), preferred_element_type=jnp.float32
    )
    dquery = turned.T.astype(jnp.bfloat16)
    for h in range(group_heads):
        dquery_ref[:, h * HEAD : (h + 1) * HEAD] = dquery[h * shard_rows : (h + 1) * shard_rows]
    middle = count * shard_rows // 2
    dkey, dvalue = dkey.astype(jnp.bfloat16), dvalue.astype(jnp.bfloat16)
    keep_k[...], send_k[...] = dkey[:middle], dkey[middle:]
    keep_v[...], send_v[...] = dvalue[:middle], dvalue[middle:]


def attention(meta, pieces, queries, out_grad, first_head, heads, group_heads, blk_count):
    count = len(pieces)
    shard_rows = queries.shape[0]
    width = group_heads * HEAD
    total = count * shard_rows

    def column(offset):
        return pl.BlockSpec((shard_rows, HEAD), lambda g, m: (0, offset + g))

    wide = pl.BlockSpec((shard_rows, width), lambda g, m: (0, first_head + g))
    half_key = pl.BlockSpec((total // 2, HEAD), lambda g, m: (0, g))
    half_shape = jax.ShapeDtypeStruct((total // 2, heads * HEAD), jnp.bfloat16)
    area = heads * group_heads * shard_rows * total
    return pl.pallas_call(
        functools.partial(
            attention_kernel, count, blk_count, group_heads, 1.0 / math.sqrt(HEAD)
        ),
        grid_spec=pltpu.PrefetchScalarGridSpec(
            num_scalar_prefetch=1,
            grid=(heads,),
            in_specs=[column(0)] * count + [column(heads)] * count + [wide, wide],
            out_specs=[
                pl.BlockSpec((shard_rows, width), lambda g, m: (0, g)),
                half_key,
                half_key,
                half_key,
                half_key,
            ],
            scratch_shapes=[pltpu.VMEM((total, shard_rows), jnp.float32)],
        ),
        out_shape=[jax.ShapeDtypeStruct((shard_rows, heads * width), jnp.bfloat16)]
        + [half_shape] * 4,
        compiler_params=pltpu.CompilerParams(vmem_limit_bytes=VMEM_LIMIT),
        cost_estimate=cost(10 * area * HEAD, 4 * shard_rows * heads * width, area),
        name="attention",
    )(meta, *pieces, *pieces, queries, out_grad)


def weight_kernel(count, *refs):
    turned = jnp.concatenate([r[...] for r in refs[:count]], 1)
    grads = jnp.concatenate([r[...] for r in refs[count : 2 * count]], 0)
    keep_ref, send_ref = refs[2 * count :]
    total = jnp.dot(turned, grads, preferred_element_type=jnp.float32)
    half = turned.shape[0] // 2
    keep_ref[...] = total[:half]
    send_ref[...] = total[half:].astype(jnp.bfloat16)


def weight_partial(turned, grads):
    count = len(turned)
    features, rows = turned[0].shape
    columns = grads[0].shape[1]
    return pl.pallas_call(
        functools.partial(weight_kernel, count),
        out_shape=[
            jax.ShapeDtypeStruct((features // 2, columns), jnp.float32),
            jax.ShapeDtypeStruct((features // 2, columns), jnp.bfloat16),
        ],
        compiler_params=pltpu.CompilerParams(vmem_limit_bytes=VMEM_LIMIT),
        cost_estimate=cost(2 * features * rows * count * columns, 4 * features * columns),
        name="weight",
    )(*turned, *grads)


def body(queries, keys, values, out_grad, layer_input, lengths):
    blk_count, dp_count = lax.axis_size("blk"), lax.axis_size("dp")
    blk_index = lax.axis_index("blk")
    linear = lax.axis_index("dp") * blk_count + blk_index
    send = Exchange(dp_count, blk_count)
    blk_bits = list(range(send.blk_bits))
    dp_bits = list(range(send.blk_bits, (dp_count * blk_count).bit_length() - 1))
    gather_bits = [dp_bits[1], dp_bits[0], blk_bits[0]]
    reduce_bits = blk_bits[1:] + dp_bits[2:]
    shard_rows = queries.shape[1]
    kv_heads = keys.shape[2] // HEAD
    group_heads = queries.shape[2] // keys.shape[2]
    key_cols = kv_heads * HEAD

    masks = [spread(i, blk_bits) for i in range(blk_count)]
    meta = jnp.stack([blk_index ^ m for m in masks] + [lengths[0, 0], lengths[0, 1]])
    meta = meta.astype(jnp.int32)

    table = jnp.array(
        [
            [spread(m, gather_bits) ^ spread(r, reduce_bits) for r in range(1 << len(reduce_bits))]
            for m in range(1 << len(gather_bits))
        ],
        jnp.int32,
    )
    turned = turned_input(layer_input[0], table ^ linear)
    turned = [turned[0]] + [
        send(turned[m], spread(m, gather_bits)) for m in range(1, len(turned))
    ]

    own_rows = blk_index * shard_rows + jnp.arange(shard_rows, dtype=jnp.int32)
    own_pos = stored_positions(own_rows, shard_rows, blk_count)
    half_dim = HEAD // 2
    frequency = jnp.exp(
        -(2.0 * jnp.arange(half_dim, dtype=jnp.float32) / HEAD) * math.log(rope_base)
    )
    angles = own_pos.astype(jnp.float32)[:, None] * frequency[None, :]
    cosine = jnp.concatenate([jnp.cos(angles), jnp.cos(angles)], axis=-1)[:, None, :]
    sine = jnp.concatenate([jnp.sin(angles), jnp.sin(angles)], axis=-1)[:, None, :]

    heads = kv_heads // CHUNKS
    query_out, key_out, value_out, weight_out = [], [], [], []
    for chunk in range(CHUNKS):
        first = chunk * heads
        cols = slice(first * HEAD, (first + heads) * HEAD)
        pair = jnp.concatenate([keys[0][:, cols], values[0][:, cols]], axis=1)
        pieces = {0: pair}
        for bit in reversed(blk_bits):
            for m, piece in list(pieces.items()):
                pieces[m | 1 << bit] = send(piece, 1 << bit)
        dquery, keep_k, keep_v, send_k, send_v = attention(
            meta, [pieces[m] for m in masks], queries[0], out_grad[0], first, heads,
            group_heads, blk_count,
        )
        query_out.append(dquery)
        kept = jnp.concatenate([keep_k, keep_v], axis=1).astype(jnp.float32)
        sent = jnp.concatenate([send_k, send_v], axis=1)
        for step, bit in enumerate(blk_bits):
            kept = kept + send(sent, 1 << bit).astype(jnp.float32)
            if step + 1 < len(blk_bits):
                middle = kept.shape[0] // 2
                kept, sent = kept[:middle], kept[middle:].astype(jnp.bfloat16)
        width = heads * HEAD
        key_sum, value_half = kept[:, :width], kept[:, width:].astype(jnp.bfloat16)
        key_out.append(key_sum.astype(jnp.bfloat16))
        value_out.append(value_half)
        grad_heads = key_sum.reshape(shard_rows, heads, HEAD)
        rotated = jnp.concatenate(
            [-grad_heads[..., half_dim:], grad_heads[..., :half_dim]], axis=-1
        )
        key_pre = (grad_heads * cosine - rotated * sine).reshape(shard_rows, width)
        grads = {0: jnp.concatenate([key_pre.astype(jnp.bfloat16), value_half], axis=1)}
        chip_bits = gather_bits[:-1]
        for i in range(1, 1 << len(chip_bits)):
            mask = spread(i, chip_bits)
            grads[mask] = send(grads[0], mask)
        core_mask = 1 << gather_bits[-1]
        for mask, piece in list(grads.items()):
            grads[mask | core_mask] = send(piece, core_mask)
        keep, sent = weight_partial(
            turned, [grads[spread(m, gather_bits)] for m in range(len(turned))]
        )
        for step, bit in enumerate(reduce_bits):
            keep = keep + send(sent, 1 << bit).astype(jnp.float32)
            if step + 1 < len(reduce_bits):
                middle = keep.shape[0] // 2
                keep, sent = keep[:middle], keep[middle:].astype(jnp.bfloat16)
        weight_out.append(keep)

    def joined(parts):
        return parts[0] if len(parts) == 1 else jnp.concatenate(parts, axis=1)

    width = heads * HEAD
    weight_grad = joined([w[:, :width] for w in weight_out] + [w[:, width:] for w in weight_out])
    if CHUNKS == 1:
        weight_grad = weight_out[0]
    return (
        joined(query_out)[None],
        joined(key_out)[None],
        joined(value_out)[None],
        weight_grad,
    )


def solution(mesh):
    token_split = P("dp", "blk", None)
    return jax.shard_map(
        body,
        mesh=mesh,
        in_specs=(token_split,) * 5 + (P("dp", None),),
        out_specs=(token_split,) * 3 + (P(("dp", "blk"), None),),
        check_vma=False,
    )
```

```python
import functools
import math

import jax
import jax.numpy as jnp
from jax import lax
from jax.experimental import pallas as pl
from jax.experimental.pallas import tpu as pltpu
from jax.sharding import PartitionSpec as P


HEAD = 128
rope_base = 500000.0
masked_fill = -1e30
LOG2E = math.log2(math.e)
CHUNKS = 2


def stored_positions(stored_rows, shard_rows, shard_count):
    half_rows = shard_rows // 2
    block_number = stored_rows // half_rows
    holder = block_number // 2
    upper_half = block_number % 2
    position_block = jnp.where(upper_half == 1, 2 * shard_count - 1 - holder, holder)
    return (position_block * half_rows + stored_rows % half_rows).astype(jnp.int32)


def spread(index, bits):
    width = len(bits)
    return sum(((index >> (width - 1 - i)) & 1) << bits[i] for i in range(width))


class Exchange:
    def __init__(self, dp_count, blk_count):
        self.dp_count, self.blk_count = dp_count, blk_count
        self.blk_bits = blk_count.bit_length() - 1

    def __call__(self, array, mask):
        blk_mask, dp_mask = mask % self.blk_count, mask // self.blk_count
        if dp_mask == 0:
            return lax.ppermute(array, "blk", [(b, b ^ blk_mask) for b in range(self.blk_count)])
        if blk_mask == 0:
            return lax.ppermute(array, "dp", [(d, d ^ dp_mask) for d in range(self.dp_count)])
        total = self.dp_count * self.blk_count
        return lax.ppermute(array, ("dp", "blk"), [(i, i ^ mask) for i in range(total)])


def cost(flops, nbytes, trans=0):
    return pl.CostEstimate(flops=int(flops), bytes_accessed=int(nbytes), transcendentals=int(trans))


def turn_kernel(masks, blk_count, rows_ref, *out_refs):
    linear = lax.axis_index("dp") * blk_count + lax.axis_index("blk")
    share = out_refs[0].shape[0] // len(masks[0])
    for m, out_ref in enumerate(out_refs):
        for r, mask in enumerate(masks[m]):
            start = pl.multiple_of((linear ^ mask) * share, share)
            out_ref[r * share : (r + 1) * share, :] = rows_ref[:, pl.ds(start, share)].T


def turned_input(rows, masks, linear, blk_count):
    row_count, features = rows.shape
    dests, blocks = len(masks), len(masks[0])
    share = features // (dests * blocks)
    if share % 128:
        turned = rows.T.reshape(dests * blocks, share, row_count)
        table = jnp.array(masks, jnp.int32) ^ linear
        return [turned[table[m]].reshape(blocks * share, row_count) for m in range(dests)]
    return pl.pallas_call(
        functools.partial(turn_kernel, masks, blk_count),
        out_shape=[jax.ShapeDtypeStruct((blocks * share, row_count), rows.dtype)] * dests,
        compiler_params=pltpu.CompilerParams(vmem_limit_bytes=8 << 20),
        cost_estimate=cost(2e9, 2 * rows.size * 2),
        name="turn",
    )(rows)


def attention_kernel(masks, blk_count, group_heads, scale, lengths_ref, *refs):
    count = len(masks)
    pair_refs = refs[:count]
    query_ref, grad_ref, dquery_ref, keep_ref, send_ref, bias_ref = refs[count:]
    shard_rows = query_ref.shape[0]
    half = shard_rows // 2

    @pl.when(pl.program_id(0) == 0)
    def _():
        def positions(shard, local):
            low = shard * half + local
            high = (2 * blk_count - 1 - shard) * half + local - half
            return jnp.where(local < half, low, high)

        own = lax.axis_index("blk")
        prompt = lengths_ref[0, 0]
        reject = prompt + lengths_ref[0, 1]
        shape = (shard_rows, shard_rows)
        query_pos = positions(own, lax.broadcasted_iota(jnp.int32, shape, 1))
        local = lax.broadcasted_iota(jnp.int32, shape, 0)
        for i, mask in enumerate(masks):
            key_pos = positions(own ^ mask, local)
            chosen = (key_pos >= prompt) & (key_pos < reject)
            blocked = (key_pos > query_pos) | ((query_pos >= reject) & chosen)
            bias_ref[i * shard_rows : (i + 1) * shard_rows, :] = jnp.where(
                blocked, masked_fill, 0.0
            )

    def stacked(ref):
        return jnp.concatenate([ref[:, h * HEAD : (h + 1) * HEAD] for h in range(group_heads)], 0)

    query, grad = stacked(query_ref), stacked(grad_ref)
    key = jnp.concatenate([r[:, :HEAD] for r in pair_refs], 0)
    value = jnp.concatenate([r[:, HEAD:] for r in pair_refs], 0)
    contract_last = (((1,), (1,)), ((), ()))
    scores = lax.dot_general(key, query, contract_last, preferred_element_type=jnp.float32)
    prob_grad = lax.dot_general(value, grad, contract_last, preferred_element_type=jnp.float32)
    bias = bias_ref[...]
    scores = scores * (scale * LOG2E) + jnp.concatenate([bias] * group_heads, 1)
    row_max = jnp.max(scores, axis=0, keepdims=True)
    weights = jnp.exp2(scores - row_max)
    inverse = 1.0 / jnp.sum(weights, axis=0, keepdims=True)
    probs = weights * inverse
    delta = jnp.sum(probs * prob_grad, axis=0, keepdims=True)
    score_grad = ((probs * scale) * (prob_grad - delta)).astype(jnp.bfloat16)
    prob_half = probs.astype(jnp.bfloat16)
    plain = (((1,), (0,)), ((), ()))
    dvalue = lax.dot_general(prob_half, grad, plain, preferred_element_type=jnp.float32)
    dkey = lax.dot_general(score_grad, query, plain, preferred_element_type=jnp.float32)
    turned = lax.dot_general(
        key, score_grad, (((0,), (0,)), ((), ())), preferred_element_type=jnp.float32
    )
    dquery = turned.T.astype(jnp.bfloat16)
    for h in range(group_heads):
        dquery_ref[:, h * HEAD : (h + 1) * HEAD] = dquery[h * shard_rows : (h + 1) * shard_rows]
    middle = count * shard_rows // 2
    dkey, dvalue = dkey.astype(jnp.bfloat16), dvalue.astype(jnp.bfloat16)
    keep_ref[:, :HEAD], keep_ref[:, HEAD:] = dkey[:middle], dvalue[:middle]
    send_ref[:, :HEAD], send_ref[:, HEAD:] = dkey[middle:], dvalue[middle:]


def attention(lengths, pieces, masks, queries, out_grad, first_head, heads, group_heads, blk_count):
    count = len(pieces)
    shard_rows = queries.shape[0]
    width = group_heads * HEAD
    total = count * shard_rows
    wide = pl.BlockSpec((shard_rows, width), lambda g: (0, first_head + g))
    half_pair = pl.BlockSpec((total // 2, 2 * HEAD), lambda g: (0, g))
    half_shape = jax.ShapeDtypeStruct((total // 2, 2 * heads * HEAD), jnp.bfloat16)
    area = heads * group_heads * shard_rows * total
    room = (8 << 20) + 10 * 4 * total * width // 2
    return pl.pallas_call(
        functools.partial(
            attention_kernel, masks, blk_count, group_heads, 1.0 / math.sqrt(HEAD)
        ),
        grid=(heads,),
        in_specs=[pl.BlockSpec(memory_space=pltpu.SMEM)]
        + [pl.BlockSpec((shard_rows, 2 * HEAD), lambda g: (0, g))] * count
        + [wide, wide],
        out_specs=[
            pl.BlockSpec((shard_rows, width), lambda g: (0, g)),
            half_pair,
            half_pair,
        ],
        scratch_shapes=[pltpu.VMEM((total, shard_rows), jnp.float32)],
        out_shape=[
            jax.ShapeDtypeStruct((shard_rows, heads * width), jnp.bfloat16),
            half_shape,
            half_shape,
        ],
        compiler_params=pltpu.CompilerParams(vmem_limit_bytes=room),
        cost_estimate=cost(30 * area * HEAD, 4 * shard_rows * heads * width, area),
        name="attention",
    )(lengths, *pieces, queries, out_grad)


def finish_kernel(kept_ref, got_ref, cos_ref, sin_ref, cols_ref, key_ref, value_ref):
    heads = key_ref.shape[1] // HEAD
    for g in range(heads):
        key_cols = slice(2 * g * HEAD, (2 * g + 1) * HEAD)
        value_cols = slice((2 * g + 1) * HEAD, (2 * g + 2) * HEAD)
        out_cols = slice(g * HEAD, (g + 1) * HEAD)
        key_sum = kept_ref[:, key_cols] + got_ref[:, key_cols].astype(jnp.float32)
        value_sum = kept_ref[:, value_cols] + got_ref[:, value_cols].astype(jnp.float32)
        value_half = value_sum.astype(jnp.bfloat16)
        swapped = pltpu.roll(key_sum, HEAD // 2, 1)
        key_pre = key_sum * cos_ref[...] + swapped * sin_ref[...]
        cols_ref[:, key_cols] = key_pre.astype(jnp.bfloat16)
        cols_ref[:, value_cols] = value_half
        key_ref[:, out_cols] = key_sum.astype(jnp.bfloat16)
        value_ref[:, out_cols] = value_half


def finish(kept, got, cosine, sine):
    rows, columns = kept.shape
    half = jax.ShapeDtypeStruct((rows, columns // 2), jnp.bfloat16)
    return pl.pallas_call(
        finish_kernel,
        out_shape=[jax.ShapeDtypeStruct((rows, columns), jnp.bfloat16), half, half],
        compiler_params=pltpu.CompilerParams(vmem_limit_bytes=4 << 20),
        cost_estimate=cost(2e8, 10 * rows * columns),
        name="finish",
    )(kept, got, cosine, sine)


def weight_kernel(count, *refs):
    turned = jnp.concatenate([r[...] for r in refs[:count]], 1)
    grads = jnp.concatenate([r[...] for r in refs[count : 2 * count]], 0)
    keep_ref, send_ref = refs[2 * count :]
    total = jnp.dot(turned, grads, preferred_element_type=jnp.float32)
    half = turned.shape[0] // 2
    keep_ref[...] = total[:half]
    send_ref[...] = total[half:].astype(jnp.bfloat16)


def weight_partial(turned, grads):
    count = len(turned)
    features, rows = turned[0].shape
    columns = grads[0].shape[1]
    return pl.pallas_call(
        functools.partial(weight_kernel, count),
        out_shape=[
            jax.ShapeDtypeStruct((features // 2, columns), jnp.float32),
            jax.ShapeDtypeStruct((features // 2, columns), jnp.bfloat16),
        ],
        compiler_params=pltpu.CompilerParams(vmem_limit_bytes=16 << 20),
        cost_estimate=cost(6 * features * rows * count * columns, 4 * features * columns),
        name="weight",
    )(*turned, *grads)


def gather_kernel(chunks, *refs):
    out_ref = refs[2 * chunks]
    heads = out_ref.shape[1] // (2 * HEAD * chunks)
    for c in range(chunks):
        keep_ref, got_ref = refs[2 * c], refs[2 * c + 1]
        for g in range(heads):
            for part in range(2):
                source = slice((2 * g + part) * HEAD, (2 * g + part + 1) * HEAD)
                place = (part * chunks * heads + c * heads + g) * HEAD
                out_ref[:, place : place + HEAD] = keep_ref[:, source] + got_ref[
                    :, source
                ].astype(jnp.float32)


def gathered(parts):
    rows, columns = parts[0][0].shape
    flat = [array for part in parts for array in part]
    return pl.pallas_call(
        functools.partial(gather_kernel, len(parts)),
        out_shape=jax.ShapeDtypeStruct((rows, columns * len(parts)), jnp.float32),
        compiler_params=pltpu.CompilerParams(vmem_limit_bytes=8 << 20),
        cost_estimate=cost(1e8, 10 * rows * columns * len(parts)),
        name="assemble",
    )(*flat)


def whole_step(queries, keys, values, out_grad, layer_input, lengths):
    blk_count, dp_count = lax.axis_size("blk"), lax.axis_size("dp")
    blk_index = lax.axis_index("blk")
    linear = lax.axis_index("dp") * blk_count + blk_index
    exchange = Exchange(dp_count, blk_count)
    blk_bits = list(range(exchange.blk_bits))
    dp_bits = list(range(exchange.blk_bits, (dp_count * blk_count).bit_length() - 1))
    gather_bits = [dp_bits[1], dp_bits[0], blk_bits[0]]
    reduce_bits = blk_bits[1:] + dp_bits[2:]
    shard_rows = queries.shape[1]
    kv_heads = keys.shape[2] // HEAD
    group_heads = queries.shape[2] // keys.shape[2]
    heads = kv_heads // CHUNKS

    own_rows = blk_index * shard_rows + jnp.arange(shard_rows, dtype=jnp.int32)
    own_pos = stored_positions(own_rows, shard_rows, blk_count)
    half_dim = HEAD // 2
    frequency = jnp.exp(
        -(2.0 * jnp.arange(half_dim, dtype=jnp.float32) / HEAD) * math.log(rope_base)
    )
    angles = own_pos.astype(jnp.float32)[:, None] * frequency[None, :]
    cosine = jnp.concatenate([jnp.cos(angles), jnp.cos(angles)], axis=-1)
    sine = jnp.concatenate([jnp.sin(angles), -jnp.sin(angles)], axis=-1)

    pairs = []
    for chunk in range(CHUNKS):
        parts = []
        for g in range(chunk * heads, (chunk + 1) * heads):
            cols = slice(g * HEAD, (g + 1) * HEAD)
            parts += [keys[0][:, cols], values[0][:, cols]]
        pairs.append({0: jnp.concatenate(parts, axis=1)})
    for pieces in pairs:
        for bit in reversed(blk_bits):
            for m, piece in list(pieces.items()):
                pieces[m | 1 << bit] = exchange(piece, 1 << bit)

    block_masks = [
        [spread(m, gather_bits) ^ spread(r, reduce_bits) for r in range(1 << len(reduce_bits))]
        for m in range(1 << len(gather_bits))
    ]
    turned = turned_input(layer_input[0], block_masks, linear, blk_count)
    turned = [turned[0]] + [
        exchange(turned[m], spread(m, gather_bits)) for m in range(1, len(turned))
    ]

    masks = [spread(i, blk_bits) for i in range(blk_count)]
    query_out, key_out, value_out, weight_out = [], [], [], []
    for chunk, pieces in enumerate(pairs):
        dquery, kept, sent = attention(
            lengths, [pieces[m] for m in masks], masks, queries[0], out_grad[0],
            chunk * heads, heads, group_heads, blk_count,
        )
        query_out.append(dquery)
        for step, bit in enumerate(blk_bits):
            got = exchange(sent, 1 << bit)
            if step + 1 < len(blk_bits):
                kept = kept.astype(jnp.float32) + got.astype(jnp.float32)
                middle = kept.shape[0] // 2
                kept, sent = kept[:middle], kept[middle:].astype(jnp.bfloat16)
        columns, key_half, value_half = finish(kept, got, cosine, sine)
        key_out.append(key_half)
        value_out.append(value_half)
        grads = {0: columns}
        chip_bits = gather_bits[:-1]
        for i in range(1, 1 << len(chip_bits)):
            mask = spread(i, chip_bits)
            grads[mask] = exchange(columns, mask)
        core_mask = 1 << gather_bits[-1]
        for mask, piece in list(grads.items()):
            grads[mask | core_mask] = exchange(piece, core_mask)
        kept, sent = weight_partial(
            turned, [grads[spread(m, gather_bits)] for m in range(len(turned))]
        )
        for step, bit in enumerate(reduce_bits):
            got = exchange(sent, 1 << bit)
            if step + 1 < len(reduce_bits):
                kept = kept + got.astype(jnp.float32)
                middle = kept.shape[0] // 2
                kept, sent = kept[:middle], kept[middle:].astype(jnp.bfloat16)
        weight_out.append((kept, got))

    def joined(parts):
        return parts[0] if len(parts) == 1 else jnp.concatenate(parts, axis=1)

    weight_grad = gathered(weight_out)
    return (
        joined(query_out)[None],
        joined(key_out)[None],
        joined(value_out)[None],
        weight_grad,
    )


def solution(mesh):
    token_split = P("dp", "blk", None)
    return jax.shard_map(
        whole_step,
        mesh=mesh,
        in_specs=(token_split,) * 5 + (P("dp", None),),
        out_specs=(token_split,) * 3 + (P(("dp", "blk"), None),),
        check_vma=False,
    )
```
